32 devices in a mesh: group: 4 (over y, core), freq: 8 (over z, x).
Axes of the slice: x: 2, y: 2, z: 4, core: 2. Of those that a mesh axis runs over, the one named last changes fastest.
Arguments:
- spectra: bfloat16 [2048, 2, 16], P('freq', None, 'group'), may hold values from -6 to 6
- templates: bfloat16 [2048, 2, 2560], P('freq', None, 'group'), may hold values from -600 to 600
- valid_start: int32 [16], replicated, may hold values from 0 to 2048
Outputs:
- peaks: float32 [2560, 16], P('group')
The draws below stay inside these ranges and needn't reach their ends.
All inputs are finite; a program needn't handle non-finite values.
Results may differ from the reference program's by a relative error of at most 0.0019.
Values may be sent and summed in bfloat16 or wider, within the bound.
No kernel may reach another device: no remote copies, remote signals or barrier semaphores. Data moves between devices by JAX's collectives and lax.ppermute only.
A program may use at most 256 MiB of HBM per device.

```python
import math
import jax
import jax.numpy as jnp
from jax import lax

N = 4096
K = 2048
VALID = 2048
SEG = 16
TEMPLATES = 2560


def draw_templates(key, part):
    base_key, row_key, col_key = jax.random.split(jax.random.fold_in(key, 11), 3)
    base = jnp.clip(jax.random.normal(base_key, (K, 2, TEMPLATES), jnp.float32), -6.0, 6.0)
    row_scale = jnp.exp(jax.random.uniform(row_key, (TEMPLATES,), jnp.float32, 0.0, math.log(10.0)))
    col_scale = jnp.exp(jax.random.uniform(col_key, (K,), jnp.float32, 0.0, math.log(10.0)))
    return (base * row_scale[None, None, :] * col_scale[:, None, None]).astype(jnp.bfloat16)


def with_ends(values, own_key, smallest, top_value):
    spot = [jax.random.randint(jax.random.fold_in(own_key, axis), (), 0, length) for axis, length in enumerate(values.shape)]
    widest = values.shape.index(max(values.shape))
    beside = spot[:widest] + [(spot[widest] + 1) % values.shape[widest]] + spot[widest + 1:]
    return values.at[tuple(spot)].set(smallest).at[tuple(beside)].set(top_value)


def steps_of(own_key, extent, cuts, smallest, high):
    factor_of = 1.0
    for position, blocks in cuts:
        heights = jax.random.uniform(jax.random.fold_in(jax.random.fold_in(own_key, 6), position), (blocks,), jnp.float32, smallest / len(cuts), high / len(cuts))
        factor_of = factor_of * jnp.repeat(jnp.exp(heights), extent[position] // blocks).reshape((-1,) + (1,) * (len(extent) - 1 - position))
    return factor_of


def noise(own_key, shape, deviation, most, cuts=(), kind=jnp.bfloat16):
    array = jax.random.normal(own_key, shape, jnp.float32) * deviation
    if len(cuts) > 0:
        array = steps_of(own_key, shape, cuts, -0.22, 0.18) * array
    return jnp.clip(array, min=-most, max=most).astype(kind)


def setup_inputs(seed: int = 0) -> dict:
    seeds = jax.random.split(jax.random.key(seed), 4)
    return {
        "spectra": noise(seeds[0], (K, 2, SEG), 1.0, 6.0, ((0, 8), (2, 4))),
        "templates": draw_templates(jax.random.fold_in(seeds[3], 71), 0),
        "valid_start": with_ends(jax.random.randint(seeds[2], (SEG,), 0, N - VALID + 1), jax.random.fold_in(seeds[2], 1), 0, N - VALID).astype(jnp.int32),
    }


def reference(spectra, templates, valid_start):
    bank = jnp.transpose(templates, (1, 2, 0)).astype(jnp.float32)
    strain_all = jnp.transpose(spectra, (1, 2, 0))
    template_norm = jnp.sum(bank[0] * bank[0] + bank[1] * bank[1], axis=1)
    bins_index = jnp.arange(K, dtype=jnp.int32)
    lag_index = jnp.arange(N, dtype=jnp.int32)
    angle = ((bins_index[:, None] * lag_index[None, :]) % N).astype(jnp.float32) * (2.0 * math.pi / N)
    cosine = jnp.cos(angle)
    sine_part = jnp.sin(angle)
    table = jnp.concatenate([jnp.concatenate([cosine, sine_part], 1), jnp.concatenate([-sine_part, cosine], 1)], 0).astype(jnp.bfloat16)

    def one_segment(segment):
        strain = lax.dynamic_index_in_dim(strain_all, segment, 1, False).astype(jnp.float32)
        cross_re = bank[0] * strain[0][None, :] + bank[1] * strain[1][None, :]
        cross_im = bank[0] * strain[1][None, :] - bank[1] * strain[0][None, :]
        cross = jnp.concatenate([cross_re, cross_im], 1).astype(jnp.bfloat16)
        series = jnp.dot(cross, table, preferred_element_type=jnp.float32)
        power = (series[:, :N] * series[:, :N] + series[:, N:] * series[:, N:]) / template_norm[:, None]
        first = valid_start[segment]
        inside = (lag_index >= first) & (lag_index < first + VALID)
        return jnp.max(jnp.where(inside[None, :], power, jnp.float32(0.0)), axis=1)

    peaks = lax.map(one_segment, jnp.arange(SEG, dtype=jnp.int32))
    return peaks.T
```

```python
import math

import jax
import jax.numpy as jnp
import numpy as np
from jax import lax
from jax.experimental import pallas as pl
from jax.experimental.pallas import tpu as pltpu
from jax.sharding import PartitionSpec as P

N = 4096
VALID = 2048
RADIX = 8
LANES = 128


def twiddles(bins):
    span = N // RADIX
    rows = bins // RADIX // 16
    t1 = np.arange(span)[None, :]
    fine = 2.0 * math.pi * ((np.arange(16)[:, None] * t1) % span) / span
    coarse = 2.0 * math.pi * ((16 * np.arange(rows)[:, None] * t1) % span) / span
    low = 2.0 * math.pi * ((np.arange(RADIX)[:, None] * t1) % N) / N
    both = lambda angle: np.stack([np.cos(angle), np.sin(angle)]).astype(np.float32)
    return both(fine), both(coarse).swapaxes(0, 1), both(low)


def transform(recv, valid_start, tpl_count):
    sources, rows_all, local = recv.shape
    segs = rows_all - tpl_count
    piece = local // (2 * RADIX)
    per_class = sources * piece
    bins = per_class * RADIX
    span = N // RADIX
    half = span // 2
    tpl_pad = -(-tpl_count // 16) * 16
    block_segs = max(d for d in range(1, segs + 1) if segs % (2 * d) == 0 and (d == 1 or d * tpl_pad <= 400))
    blocks = segs // block_segs
    rows = block_segs * tpl_pad
    tiles = per_class // LANES
    fine, coarse, low = twiddles(bins)
    pad = tpl_pad - tpl_count
    if pad:
        recv = jnp.concatenate(
            [recv[:, :tpl_count], jnp.zeros((sources, pad, local), recv.dtype), recv[:, tpl_count:]], 1
        )
    rows_all = tpl_pad + segs
    root = np.float32(math.sqrt(0.5))

    def kernel(start_ref, recv_ref, fine_ref, coarse_ref, low_ref, out_ref, wide, strain, table, xa, xb, ya, yb, acc):
        def table_rows(a, carry):
            cr = coarse_ref[a, 0:1, :]
            ci = coarse_ref[a, 1:2, :]
            ar = cr * fine_ref[0] - ci * fine_ref[1]
            ai = cr * fine_ref[1] + ci * fine_ref[0]
            at = pl.multiple_of(a * 16, 16)
            for k2 in range(RADIX):
                lr = low_ref[0, k2 : k2 + 1, :]
                li = low_ref[1, k2 : k2 + 1, :]
                c = ar * lr - ai * li
                s = ar * li + ai * lr
                cb = c.astype(jnp.bfloat16)
                sb = s.astype(jnp.bfloat16)
                nb = (-s).astype(jnp.bfloat16)
                for ph in range(2):
                    col = ph * span
                    t = slice(ph * half, (ph + 1) * half)
                    table[k2, pl.ds(at, 16), col : col + half] = cb[:, t]
                    table[k2, pl.ds(at, 16), col + half : col + span] = sb[:, t]
                    table[k2, pl.ds(per_class + at, 16), col : col + half] = nb[:, t]
                    table[k2, pl.ds(per_class + at, 16), col + half : col + span] = cb[:, t]
            return carry

        lax.fori_loop(0, per_class // 16, table_rows, 0)

        lane = lax.broadcasted_iota(jnp.int32, (rows_all, LANES), 1)
        per_tile = LANES // piece
        for k2 in range(RADIX):
            for c in range(2):
                lane0 = k2 * 2 * piece + c * piece
                tile, inner = lane0 // LANES, lane0 % LANES
                for j in range(tiles):
                    value = None
                    for i in range(per_tile):
                        part = recv_ref[j * per_tile + i, :, tile * LANES : (tile + 1) * LANES].astype(jnp.float32)
                        shift = (i * piece - inner) % LANES
                        if shift:
                            part = pltpu.roll(part, shift, 1)
                        value = part if value is None else jnp.where(lane >= i * piece, part, value)
                    at = k2 * per_class + j * LANES
                    wide[c, :, at : at + LANES] = value

        for s in range(segs):
            for c in range(2):
                strain[s, c : c + 1, :] = wide[c, tpl_pad + s : tpl_pad + s + 1, :]

        def cross_piece(x_ref, block, index):
            tile, i = index // block_segs, index % block_segs
            k2, j = tile // tiles, tile % tiles
            at = slice(tile * LANES, (tile + 1) * LANES)
            seg = block * block_segs + i
            d0 = strain[seg, 0:1, at]
            d1 = strain[seg, 1:2, at]
            col = k2 * 2 * per_class + j * LANES
            for t in range(0, tpl_pad, 16):
                h0 = wide[0, t : t + 16, at]
                h1 = wide[1, t : t + 16, at]
                row = slice(i * tpl_pad + t, i * tpl_pad + t + 16)
                x_ref[row, col : col + LANES] = (h0 * d0 + h1 * d1).astype(jnp.bfloat16)
                col_im = col + per_class
                x_ref[row, col_im : col_im + LANES] = (h0 * d1 - h1 * d0).astype(jnp.bfloat16)

        cross_count = RADIX * tiles * block_segs
        lane16 = lax.broadcasted_iota(jnp.int32, (16, LANES), 1)
        lane_tiles = half // LANES
        row_tiles = tpl_pad // 16
        peak_count = block_segs * lane_tiles * row_tiles
        signs = {}

        def peak_piece(y_ref, block, phase, index, key):
            i = index // (lane_tiles * row_tiles)
            u = index // row_tiles % lane_tiles
            r = index % row_tiles
            if (key, i, u) not in signs:
                first = start_ref[block * block_segs + i] - (phase * half + u * LANES)
                one = [jnp.float32(1.0), root, jnp.float32(1.0), root]
                signs[key, i, u] = [
                    jnp.where(lane16 >= first - span * j, one[j], -one[j]) for j in range(4)
                ]
            sign = signs[key, i, u]
            row = slice(i * tpl_pad + r * 16, i * tpl_pad + r * 16 + 16)
            re = lambda k: y_ref[k, row, u * LANES : (u + 1) * LANES]
            im = lambda k: y_ref[k, row, half + u * LANES : half + (u + 1) * LANES]

            def four(a, b, c, d):
                ar, ai, br, bi, cr, ci, dr, di = re(a), im(a), re(b), im(b), re(c), im(c), re(d), im(d)
                pr, pi, qr, qi = ar + cr, ai + ci, ar - cr, ai - ci
                sr, si, wr, wi = br + dr, bi + di, br - dr, bi - di
                return (
                    (pr + sr, pi + si),
                    (qr - wi, qi + wr),
                    (pr - sr, pi - si),
                    (qr + wi, qi - wr),
                )

            even = four(0, 2, 4, 6)
            odd = four(1, 3, 5, 7)
            odd = (
                odd[0],
                (odd[1][0] - odd[1][1], odd[1][0] + odd[1][1]),
                (-odd[2][1], odd[2][0]),
                (-odd[3][0] - odd[3][1], odd[3][0] - odd[3][1]),
            )
            best = None
            for j in range(4):
                yr = even[j][0] + sign[j] * odd[j][0]
                yi = even[j][1] + sign[j] * odd[j][1]
                power = yr * yr + yi * yi
                best = power if best is None else jnp.maximum(best, power)
            if phase == 0 and u == 0:
                acc[block, row, :] = best
            else:
                acc[block, row, :] = jnp.maximum(acc[block, row, :], best)

        for index in range(cross_count):
            cross_piece(xa, 0, index)

        def phase_step(x_ref, y_new, phase, y_old, old_block, old_phase, x_next, next_block, key):
            share_p = -(-peak_count // RADIX)
            share_c = -(-(cross_count // 2) // RADIX)
            for k2 in range(RADIX):
                y_new[k2] = jnp.dot(
                    x_ref[:, k2 * 2 * per_class : (k2 + 1) * 2 * per_class],
                    table[k2, :, phase * span : (phase + 1) * span],
                    preferred_element_type=jnp.float32,
                )
                for index in range(k2 * share_p, min((k2 + 1) * share_p, peak_count)):
                    peak_piece(y_old, old_block, old_phase, index, key)
                for index in range(k2 * share_c, min((k2 + 1) * share_c, cross_count // 2)):
                    cross_piece(x_next, next_block, phase * (cross_count // 2) + index)

        def pair(p, carry):
            signs.clear()
            b = 2 * p
            last = jnp.where(p == 0, blocks, b - 1)
            after = jnp.where(b + 2 < blocks, b + 2, 0)
            phase_step(xa, ya, 0, yb, last, 1, xb, b + 1, 0)
            phase_step(xa, yb, 1, ya, b, 0, xb, b + 1, 1)
            phase_step(xb, ya, 0, yb, b, 1, xa, after, 2)
            phase_step(xb, yb, 1, ya, b + 1, 0, xa, after, 3)
            return carry

        lax.fori_loop(0, blocks // 2, pair, 0)
        signs.clear()
        for index in range(peak_count):
            peak_piece(yb, blocks - 1, 1, index, 0)

        square = wide[0, :tpl_pad, :] * wide[0, :tpl_pad, :] + wide[1, :tpl_pad, :] * wide[1, :tpl_pad, :]
        norm = jnp.sum(square, axis=1, keepdims=True)
        column = lax.broadcasted_iota(jnp.int32, (tpl_pad, segs), 1)
        result = jnp.zeros((tpl_pad, segs), jnp.float32)
        for s in range(segs):
            b, i = s // block_segs, s % block_segs
            top = jnp.max(acc[b, i * tpl_pad : (i + 1) * tpl_pad, :], axis=1, keepdims=True)
            result = jnp.where(column == s, top, result)
        out_ref[...] = result / norm

    any_vmem = pl.BlockSpec(memory_space=pltpu.VMEM)
    peaks = pl.pallas_call(
        kernel,
        out_shape=jax.ShapeDtypeStruct((tpl_pad, segs), jnp.float32),
        in_specs=[pl.BlockSpec(memory_space=pltpu.SMEM)] + [any_vmem] * 4,
        out_specs=any_vmem,
        scratch_shapes=[
            pltpu.VMEM((2, rows_all, bins), jnp.float32),
            pltpu.VMEM((segs, 2, bins), jnp.float32),
            pltpu.VMEM((RADIX, 2 * per_class, 2 * span), jnp.bfloat16),
            pltpu.VMEM((rows, 2 * bins), jnp.bfloat16),
            pltpu.VMEM((rows, 2 * bins), jnp.bfloat16),
            pltpu.VMEM((RADIX, rows, span), jnp.float32),
            pltpu.VMEM((RADIX, rows, span), jnp.float32),
            pltpu.VMEM((blocks + 1, rows, LANES), jnp.float32),
        ],
        compiler_params=pltpu.CompilerParams(vmem_limit_bytes=48 * 1024 * 1024),
        name="transform",
    )(valid_start, recv, jnp.asarray(fine), jnp.asarray(coarse), jnp.asarray(low))
    return peaks[:tpl_count]


def by_class(array):
    bins, two, columns = array.shape
    split = array.reshape(bins // RADIX, RADIX, two, columns)
    return split.transpose(3, 1, 2, 0).reshape(columns, two * bins)


def spread(block, axis):
    count = lax.axis_size(axis)
    index = lax.axis_index(axis)
    step = 1
    while step < count:
        other = lax.ppermute(block, axis, [(j, j ^ step) for j in range(count)])
        low = jnp.concatenate([block, other], 0)
        high = jnp.concatenate([other, block], 0)
        block = jnp.where((index & step) == 0, low, high)
        step *= 2
    return block


def on_device(spectra, templates, valid_start):
    freq_count = lax.axis_size("freq")
    tpl_count = templates.shape[2] // freq_count
    segments = lax.all_gather(by_class(spectra), "group", axis=0, tiled=True)
    bank = by_class(templates).reshape(freq_count, tpl_count, -1)
    every = jnp.broadcast_to(segments[None], (freq_count,) + segments.shape)
    recv = lax.all_to_all(jnp.concatenate([bank, every], 1), "freq", 0, 0, tiled=True)
    peaks = transform(recv, valid_start, tpl_count)
    return spread(peaks, "freq")


def solution(mesh):
    in_specs = (P("freq", None, "group"), P("freq", None, "group"), P())
    out_specs = P("group", None)
    return jax.shard_map(
        on_device, mesh=mesh, in_specs=in_specs, out_specs=out_specs, check_vma=False
    )
```

```python
import math

import jax
import jax.numpy as jnp
import numpy as np
from jax import lax
from jax.experimental import pallas as pl
from jax.experimental.pallas import tpu as pltpu
from jax.sharding import PartitionSpec as P


N = 4096
RADIX = 8
LANES = 128
VMEM_MIB = 52


def twiddles(bins):
    span = N // RADIX
    rows = bins // RADIX // 16
    t1 = np.arange(span)[None, :]
    fine = (np.arange(16)[:, None] * t1) % span / span
    coarse = (16 * np.arange(rows)[:, None] * t1) % span / span
    low = (np.arange(RADIX)[:, None] * t1) % N / N
    angle = 2.0 * math.pi * np.concatenate([fine, low, coarse], 0)
    return np.stack([np.cos(angle), np.sin(angle)], 1).astype(np.float32)


def make_table(bins):
    per_class = bins // RADIX
    span = N // RADIX
    half = span // 2

    def kernel(factor_ref, table, fine):
        for row in range(16):
            for c in range(2):
                fine[c, row : row + 1, :] = factor_ref[row, c : c + 1, :]

        def table_rows(a, carry):
            cr = factor_ref[16 + RADIX + a, 0:1, :]
            ci = factor_ref[16 + RADIX + a, 1:2, :]
            ar = cr * fine[0] - ci * fine[1]
            ai = cr * fine[1] + ci * fine[0]
            at = pl.multiple_of(a * 16, 16)
            for k2 in range(RADIX):
                lr = factor_ref[16 + k2, 0:1, :]
                li = factor_ref[16 + k2, 1:2, :]
                c = (ar * lr - ai * li).astype(jnp.bfloat16)
                s = (ar * li + ai * lr).astype(jnp.bfloat16)
                for ph in range(2):
                    t = slice(ph * half, (ph + 1) * half)
                    table[ph, k2, pl.ds(at, 16), :half] = c[:, t]
                    table[ph, k2, pl.ds(at, 16), half:] = s[:, t]
                    table[ph, k2, pl.ds(per_class + at, 16), :half] = -s[:, t]
                    table[ph, k2, pl.ds(per_class + at, 16), half:] = c[:, t]
            return carry

        lax.fori_loop(0, per_class // 16, table_rows, 0)

    any_vmem = pl.BlockSpec(memory_space=pltpu.VMEM)
    return pl.pallas_call(
        kernel,
        out_shape=jax.ShapeDtypeStruct((2, RADIX, 2 * per_class, span), jnp.bfloat16),
        in_specs=[any_vmem],
        out_specs=any_vmem,
        scratch_shapes=[pltpu.VMEM((2, 16, span), jnp.float32)],
        compiler_params=pltpu.CompilerParams(vmem_limit_bytes=24 * 1024 * 1024),
        name="table",
    )(jnp.asarray(twiddles(bins)))


def transform(bank, strain, place, table, valid_start):
    sources, tpl_count, local = bank.shape
    segs = strain.shape[1]
    piece = local // (2 * RADIX)
    per_class = sources * piece
    bins = per_class * RADIX
    span = N // RADIX
    half = span // 2
    tpl_pad = -(-tpl_count // 16) * 16
    block_segs = max(d for d in range(1, segs + 1) if segs % (2 * d) == 0 and (d == 1 or d * tpl_pad <= 400))
    blocks = segs // block_segs
    rows = block_segs * tpl_pad
    tiles = per_class // LANES
    if tpl_pad > tpl_count:
        bank = jnp.pad(bank, ((0, 0), (0, tpl_pad - tpl_count), (0, 0)))
    root = np.float32(math.sqrt(0.5))

    def kernel(start_hbm, bank_ref, strain_ref, table_ref, out_ref, start_ref, start_sem, table, sem, wide, lines, flat, xa, xb, ya, yb, acc):
        load = pltpu.make_async_copy(table_ref, table, sem)
        load.start()
        fetch = pltpu.make_async_copy(start_hbm, start_ref, start_sem)
        fetch.start()

        def gather(source_ref, at_of, count, store):
            lane = lax.broadcasted_iota(jnp.int32, (count, LANES), 1)
            per_tile = LANES // piece
            for j in range(tiles):
                for q in range(local // LANES):
                    parts = [
                        source_ref[at_of[j * per_tile + i], :, q * LANES : (q + 1) * LANES].astype(jnp.float32)
                        for i in range(per_tile)
                    ]
                    for inner in range(0, LANES, piece):
                        value = None
                        for i in range(per_tile):
                            shift = (i * piece - inner) % LANES
                            part = pltpu.roll(parts[i], shift, 1) if shift else parts[i]
                            value = part if value is None else jnp.where(lane >= i * piece, part, value)
                        k2, c = divmod((q * LANES + inner) // piece, 2)
                        store(c, slice(k2 * per_class + j * LANES, k2 * per_class + (j + 1) * LANES), value)

        def store_bank(c, at, value):
            wide[c, :, at] = value

        def store_lines(c, at, value):
            flat[c, :, at] = value

        gather(bank_ref, range(sources), tpl_pad, store_bank)
        gather(strain_ref, place, segs, store_lines)
        for s in range(segs):
            for c in range(2):
                lines[s, c : c + 1, :] = flat[c, s : s + 1, :]

        def cross_piece(x_ref, block, tile):
            k2, j = tile // tiles, tile % tiles
            at = slice(tile * LANES, (tile + 1) * LANES)
            col = k2 * 2 * per_class + j * LANES
            col_im = col + per_class
            d = [
                [jnp.broadcast_to(lines[block * block_segs + i, c : c + 1, at], (8, LANES)) for c in range(2)]
                for i in range(block_segs)
            ]
            for t in range(0, tpl_pad, 8):
                h0 = wide[0, t : t + 8, at]
                h1 = wide[1, t : t + 8, at]
                for i in range(block_segs):
                    row = slice(i * tpl_pad + t, i * tpl_pad + t + 8)
                    x_ref[row, col : col + LANES] = h0 * d[i][0] + h1 * d[i][1]
                    x_ref[row, col_im : col_im + LANES] = h0 * d[i][1] - h1 * d[i][0]

        cross_count = RADIX * tiles
        lane8 = lax.broadcasted_iota(jnp.int32, (8, LANES), 1)
        lane_tiles = half // LANES
        row_tiles = tpl_pad // 8
        peak_count = block_segs * lane_tiles * row_tiles
        signs = {}

        def peak_piece(y_ref, block, phase, index, key):
            i = index // (lane_tiles * row_tiles)
            u = index // row_tiles % lane_tiles
            r = index % row_tiles
            if (key, i, u) not in signs:
                first = start_ref[block * block_segs + i] - (phase * half + u * LANES)
                one = [jnp.float32(1.0), root, jnp.float32(1.0), root]
                signs[key, i, u] = [
                    jnp.where(lane8 >= first - span * j, one[j], -one[j]) for j in range(4)
                ]
            sign = signs[key, i, u]
            row = slice(i * tpl_pad + r * 8, i * tpl_pad + r * 8 + 8)
            re = lambda k: y_ref[k, row, u * LANES : (u + 1) * LANES]
            im = lambda k: y_ref[k, row, half + u * LANES : half + (u + 1) * LANES]

            def four(a, b, c, d):
                ar, ai, br, bi, cr, ci, dr, di = re(a), im(a), re(b), im(b), re(c), im(c), re(d), im(d)
                pr, pi, qr, qi = ar + cr, ai + ci, ar - cr, ai - ci
                sr, si, wr, wi = br + dr, bi + di, br - dr, bi - di
                return (
                    (pr + sr, pi + si),
                    (qr - wi, qi + wr),
                    (pr - sr, pi - si),
                    (qr + wi, qi - wr),
                )

            even = four(0, 2, 4, 6)
            odd = four(1, 3, 5, 7)
            best = None
            for j in range(4):
                er, ei = even[j]
                (a, b), g = odd[j], sign[j]
                if j == 0:
                    yr, yi = er + g * a, ei + g * b
                elif j == 1:
                    yr, yi = er + g * (a - b), ei + g * (a + b)
                elif j == 2:
                    yr, yi = er - g * b, ei + g * a
                else:
                    yr, yi = er - g * (a + b), ei + g * (a - b)
                power = yr * yr + yi * yi
                best = power if best is None else jnp.maximum(best, power)
            if phase == 0 and u == 0:
                acc[block, row, :] = best
            else:
                acc[block, row, :] = jnp.maximum(acc[block, row, :], best)

        for index in range(cross_count):
            cross_piece(xa, 0, index)

        def phase_step(x_ref, y_new, phase, y_old, old_block, old_phase, x_next, next_block, key):
            share_p = -(-peak_count // RADIX)
            share_c = -(-(cross_count // 2) // RADIX)
            for k2 in range(RADIX):
                y_new[k2] = lax.dot_general(
                    x_ref[:, k2 * 2 * per_class : (k2 + 1) * 2 * per_class],
                    table[phase, k2],
                    (((1,), (0,)), ((), ())),
                    preferred_element_type=jnp.float32,
                )
                for index in range(k2 * share_p, min((k2 + 1) * share_p, peak_count)):
                    peak_piece(y_old, old_block, old_phase, index, key)
                for index in range(k2 * share_c, min((k2 + 1) * share_c, cross_count // 2)):
                    cross_piece(x_next, next_block, phase * (cross_count // 2) + index)

        def pair(p, carry):
            signs.clear()
            b = 2 * p
            last = jnp.where(p == 0, blocks, b - 1)
            after = jnp.where(b + 2 < blocks, b + 2, 0)
            phase_step(xa, ya, 0, yb, last, 1, xb, b + 1, 0)
            phase_step(xa, yb, 1, ya, b, 0, xb, b + 1, 1)
            phase_step(xb, ya, 0, yb, b, 1, xa, after, 2)
            phase_step(xb, yb, 1, ya, b + 1, 0, xa, after, 3)
            return carry

        load.wait()
        fetch.wait()
        lax.fori_loop(0, blocks // 2, pair, 0)
        signs.clear()
        for index in range(peak_count):
            peak_piece(yb, blocks - 1, 1, index, 0)

        square = wide[0] * wide[0] + wide[1] * wide[1]
        norm = jnp.sum(square, axis=1, keepdims=True)
        column = lax.broadcasted_iota(jnp.int32, (tpl_pad, segs), 1)
        result = jnp.zeros((tpl_pad, segs), jnp.float32)
        for s in range(segs):
            b, i = s // block_segs, s % block_segs
            top = jnp.max(acc[b, i * tpl_pad : (i + 1) * tpl_pad, :], axis=1, keepdims=True)
            result = jnp.where(column == s, top, result)
        out_ref[...] = (result / norm).T

    any_vmem = pl.BlockSpec(memory_space=pltpu.VMEM)
    peaks = pl.pallas_call(
        kernel,
        out_shape=jax.ShapeDtypeStruct((segs, tpl_pad), jnp.float32),
        in_specs=[pl.BlockSpec(memory_space=pltpu.HBM)]
        + [any_vmem] * 2
        + [pl.BlockSpec(memory_space=pltpu.HBM)],
        out_specs=any_vmem,
        scratch_shapes=[
            pltpu.SMEM((segs,), jnp.int32),
            pltpu.SemaphoreType.DMA,
            pltpu.VMEM((2, RADIX, 2 * per_class, span), jnp.bfloat16),
            pltpu.SemaphoreType.DMA,
            pltpu.VMEM((2, tpl_pad, bins), jnp.float32),
            pltpu.VMEM((segs, 2, bins), jnp.float32),
            pltpu.VMEM((2, segs, bins), jnp.float32),
            pltpu.VMEM((rows, 2 * bins), jnp.float32),
            pltpu.VMEM((rows, 2 * bins), jnp.float32),
            pltpu.VMEM((RADIX, rows, span), jnp.float32),
            pltpu.VMEM((RADIX, rows, span), jnp.float32),
            pltpu.VMEM((blocks + 1, rows, LANES), jnp.float32),
        ],
        compiler_params=pltpu.CompilerParams(vmem_limit_bytes=VMEM_MIB * 1024 * 1024),
        name="transform",
    )(valid_start, bank, strain, table)
    return peaks[:, :tpl_count]


def by_class(array):
    bins, two, columns = array.shape
    split = array.reshape(bins // RADIX, RADIX, two, columns)
    return split.transpose(3, 1, 2, 0).reshape(columns, two * bins)


def swap(block, axis, bit, dim):
    index = lax.axis_index(axis)
    count = lax.axis_size(axis)
    other = lax.ppermute(block, axis, [(j, j ^ (1 << bit)) for j in range(count)])
    low = jnp.concatenate([block, other], dim)
    high = jnp.concatenate([other, block], dim)
    return jnp.where((index >> bit) & 1 == 0, low, high)


def on_device(spectra, templates, valid_start):
    freq_count = lax.axis_size("freq")
    tpl_count = templates.shape[2] // freq_count
    exchange = lambda a: lax.all_to_all(a, "freq", 0, 0, tiled=True)
    to_all = lambda a: jnp.broadcast_to(a[None], (freq_count,) + a.shape)
    bits = freq_count.bit_length() - 1
    order = [bits - 1] + list(range(bits - 1))
    strain = swap(by_class(spectra)[None], "freq", order[0], 0)
    bank = lax.optimization_barrier(by_class(templates))
    bank = exchange(bank.reshape(freq_count, tpl_count, -1))
    table = make_table(templates.shape[0] * freq_count)
    strain = swap(strain, "freq", order[1], 0)
    for bit in order[2:]:
        strain = swap(strain, "freq", bit, 0)
    for bit in range(lax.axis_size("group").bit_length() - 1):
        strain = swap(strain, "group", bit, 1)
    place = [sum(((f >> bit) & 1) << i for i, bit in enumerate(order)) for f in range(freq_count)]
    peaks = exchange(to_all(transform(bank, strain, place, table, valid_start)))
    return peaks.transpose(0, 2, 1).reshape(templates.shape[2], -1)


def solution(mesh):
    in_specs = (P("freq", None, "group"), P("freq", None, "group"), P())
    out_specs = P("group", None)
    return jax.shard_map(
        on_device, mesh=mesh, in_specs=in_specs, out_specs=out_specs, check_vma=False
    )
```

```python
import functools
import math

import jax
import jax.numpy as jnp
import numpy as np
from jax import lax
from jax.experimental import pallas as pl
from jax.experimental.pallas import tpu as pltpu
from jax.sharding import PartitionSpec as P


N = 4096
RADIX = 8
LANES = 128
VMEM_MIB = 52


def twiddles(bins):
    span = N // RADIX
    rows = bins // RADIX // 16
    t1 = np.arange(span)[None, :]
    fine = (np.arange(16)[:, None] * t1) % span / span
    coarse = (16 * np.arange(rows)[:, None] * t1) % span / span
    low = (np.arange(RADIX)[:, None] * t1) % N / N
    angle = 2.0 * math.pi * np.concatenate([fine, low, coarse], 0)
    return np.stack([np.cos(angle), np.sin(angle)], 1).astype(np.float32)


def make_table(bins):
    per_class = bins // RADIX
    span = N // RADIX
    half = span // 2
    tiles = half // LANES

    def kernel(factor_ref, table, fine):
        for row in range(16):
            for c in range(2):
                fine[c, row : row + 1, :] = factor_ref[row, c : c + 1, :]

        def table_rows(a, carry):
            cr = factor_ref[16 + RADIX + a, 0:1, :]
            ci = factor_ref[16 + RADIX + a, 1:2, :]
            ar = cr * fine[0] - ci * fine[1]
            ai = cr * fine[1] + ci * fine[0]
            at = pl.multiple_of(a * 16, 16)
            for k2 in range(RADIX):
                lr = factor_ref[16 + k2, 0:1, :]
                li = factor_ref[16 + k2, 1:2, :]
                c = (ar * lr - ai * li).astype(jnp.bfloat16)
                s = (ar * li + ai * lr).astype(jnp.bfloat16)
                for ph in range(2):
                    for u in range(tiles):
                        t = slice(ph * half + u * LANES, ph * half + (u + 1) * LANES)
                        table[ph, k2, u, pl.ds(at, 16), :] = c[:, t]
                        table[ph, k2, tiles + u, pl.ds(at, 16), :] = s[:, t]
                        table[ph, k2, u, pl.ds(per_class + at, 16), :] = -s[:, t]
                        table[ph, k2, tiles + u, pl.ds(per_class + at, 16), :] = c[:, t]
            return carry

        lax.fori_loop(0, per_class // 16, table_rows, 0)

    any_vmem = pl.BlockSpec(memory_space=pltpu.VMEM)
    return pl.pallas_call(
        kernel,
        out_shape=jax.ShapeDtypeStruct((2, RADIX, 2 * tiles, 2 * per_class, LANES), jnp.bfloat16),
        in_specs=[any_vmem],
        out_specs=any_vmem,
        scratch_shapes=[pltpu.VMEM((2, 16, span), jnp.float32)],
        compiler_params=pltpu.CompilerParams(vmem_limit_bytes=24 * 1024 * 1024),
        name="table",
    )(jnp.asarray(twiddles(bins)))


def transform(bank, strain, place, table, valid_start):
    sources, tpl_count, local = bank.shape
    segs = strain.shape[1]
    piece = local // (2 * RADIX)
    per_class = sources * piece
    bins = per_class * RADIX
    span = N // RADIX
    half = span // 2
    tpl_pad = -(-tpl_count // 16) * 16
    block_segs = max(d for d in range(1, segs + 1) if segs % (2 * d) == 0 and (d == 1 or d * tpl_pad <= 400))
    blocks = segs // block_segs
    rows = block_segs * tpl_pad
    tiles = per_class // LANES
    if tpl_pad > tpl_count:
        bank = jnp.pad(bank, ((0, 0), (0, tpl_pad - tpl_count), (0, 0)))
    root = np.float32(math.sqrt(0.5))

    def kernel(*refs):
        pl.run_scoped(
            functools.partial(body, *refs),
            pltpu.VMEM((2, RADIX, 2 * half // LANES, 2 * per_class, LANES), jnp.bfloat16),
            pltpu.VMEM((rows, 2 * bins), jnp.bfloat16),
            pltpu.VMEM((rows, 2 * bins), jnp.bfloat16),
        )

    def body(
        start_hbm, bank_ref, strain_ref, table_ref, out_ref, start_ref, start_sem, sem, wide, lines, flat, ya, yb, acc,
        table, xa, xb,
    ):
        loads = [pltpu.make_async_copy(table_ref.at[ph], table.at[ph], sem.at[ph]) for ph in range(2)]
        for load in loads:
            load.start()
        fetch = pltpu.make_async_copy(start_hbm, start_ref, start_sem)
        fetch.start()

        def gather(source_ref, at_of, count, store):
            lane = lax.broadcasted_iota(jnp.int32, (count, LANES), 1)
            per_tile = LANES // piece
            for j in range(tiles):
                for q in range(local // LANES):
                    parts = [
                        source_ref[at_of[j * per_tile + i], :, q * LANES : (q + 1) * LANES].astype(jnp.float32)
                        for i in range(per_tile)
                    ]
                    for inner in range(0, LANES, piece):
                        value = None
                        for i in range(per_tile):
                            shift = (i * piece - inner) % LANES
                            part = pltpu.roll(parts[i], shift, 1) if shift else parts[i]
                            value = part if value is None else jnp.where(lane >= i * piece, part, value)
                        k2, c = divmod((q * LANES + inner) // piece, 2)
                        store(c, slice(k2 * per_class + j * LANES, k2 * per_class + (j + 1) * LANES), value)

        def store_bank(c, at, value):
            wide[c, :, at] = value

        def store_lines(c, at, value):
            flat[c, :, at] = value

        gather(bank_ref, range(sources), tpl_pad, store_bank)
        gather(strain_ref, place, segs, store_lines)
        for s in range(segs):
            for c in range(2):
                lines[s, c : c + 1, :] = flat[c, s : s + 1, :]

        def cross_piece(x_ref, block, tile):
            k2, j = tile // tiles, tile % tiles
            at = slice(tile * LANES, (tile + 1) * LANES)
            col = k2 * 2 * per_class + j * LANES
            col_im = col + per_class
            d = [
                [jnp.broadcast_to(lines[block * block_segs + i, c : c + 1, at], (8, LANES)) for c in range(2)]
                for i in range(block_segs)
            ]
            shape = (2, 8, LANES)
            for t in range(0, tpl_pad, 16):
                h0 = wide[0, t : t + 16, at].reshape(shape)
                h1 = wide[1, t : t + 16, at].reshape(shape)
                for i in range(block_segs):
                    row = slice(i * tpl_pad + t, i * tpl_pad + t + 16)
                    re = (h0 * d[i][0] + h1 * d[i][1]).reshape(16, LANES)
                    im = (h0 * d[i][1] - h1 * d[i][0]).reshape(16, LANES)
                    x_ref[row, col : col + LANES] = re.astype(jnp.bfloat16)
                    x_ref[row, col_im : col_im + LANES] = im.astype(jnp.bfloat16)

        cross_count = RADIX * tiles
        lane8 = lax.broadcasted_iota(jnp.int32, (8, LANES), 1)
        lane_tiles = half // LANES
        row_tiles = tpl_pad // 8
        peak_count = block_segs * lane_tiles * row_tiles
        signs = {}

        def peak_piece(y_ref, block, phase, index, key):
            i = index // (lane_tiles * row_tiles)
            u = index // row_tiles % lane_tiles
            r = index % row_tiles
            if (key, i, u) not in signs:
                first = start_ref[block * block_segs + i] - (phase * half + u * LANES)
                one = [jnp.float32(1.0), root, jnp.float32(1.0), root]
                signs[key, i, u] = [
                    jnp.where(lane8 >= first - span * j, one[j], -one[j]) for j in range(4)
                ]
            sign = signs[key, i, u]
            row = slice(i * tpl_pad + r * 8, i * tpl_pad + r * 8 + 8)
            re = lambda k: y_ref[k, row, u * LANES : (u + 1) * LANES]
            im = lambda k: y_ref[k, row, half + u * LANES : half + (u + 1) * LANES]

            def four(a, b, c, d):
                ar, ai, br, bi, cr, ci, dr, di = re(a), im(a), re(b), im(b), re(c), im(c), re(d), im(d)
                pr, pi, qr, qi = ar + cr, ai + ci, ar - cr, ai - ci
                sr, si, wr, wi = br + dr, bi + di, br - dr, bi - di
                return (
                    (pr + sr, pi + si),
                    (qr - wi, qi + wr),
                    (pr - sr, pi - si),
                    (qr + wi, qi - wr),
                )

            even = four(0, 2, 4, 6)
            odd = four(1, 3, 5, 7)
            best = None
            for j in range(4):
                er, ei = even[j]
                (a, b), g = odd[j], sign[j]
                if j == 0:
                    yr, yi = er + g * a, ei + g * b
                elif j == 1:
                    yr, yi = er + g * (a - b), ei + g * (a + b)
                elif j == 2:
                    yr, yi = er - g * b, ei + g * a
                else:
                    yr, yi = er - g * (a + b), ei + g * (a - b)
                power = yr * yr + yi * yi
                best = power if best is None else jnp.maximum(best, power)
            if phase == 0 and u == 0:
                acc[block, row, :] = best
            else:
                acc[block, row, :] = jnp.maximum(acc[block, row, :], best)

        for index in range(cross_count):
            cross_piece(xa, 0, index)

        share_p = -(-peak_count // RADIX)
        share_c = -(-(cross_count // 2) // RADIX)
        x_refs, y_refs = (xa, xb), (ya, yb)
        fetch.wait()
        for step in range(2 * blocks):
            block, phase = divmod(step, 2)
            if block == 0:
                loads[phase].wait()
            signs.clear()
            for k2 in range(RADIX):
                tile = [table[phase, k2, n] for n in range(2 * lane_tiles)]
                y_refs[phase][k2, :rows, :span] = lax.dot_general(
                    x_refs[block % 2][:, k2 * 2 * per_class : (k2 + 1) * 2 * per_class],
                    jnp.concatenate(tile, 1),
                    (((1,), (0,)), ((), ())),
                    preferred_element_type=jnp.float32,
                )
                if step > 0:
                    before, before_phase = divmod(step - 1, 2)
                    for index in range(k2 * share_p, min((k2 + 1) * share_p, peak_count)):
                        peak_piece(y_refs[before_phase], before, before_phase, index, step)
                if block + 1 < blocks:
                    for index in range(k2 * share_c, min((k2 + 1) * share_c, cross_count // 2)):
                        cross_piece(x_refs[(block + 1) % 2], block + 1, phase * (cross_count // 2) + index)
        signs.clear()
        for index in range(peak_count):
            peak_piece(yb, blocks - 1, 1, index, 0)

        square = wide[0, :, :bins] * wide[0, :, :bins] + wide[1, :, :bins] * wide[1, :, :bins]
        norm = jnp.sum(square, axis=1, keepdims=True)
        column = lax.broadcasted_iota(jnp.int32, (tpl_pad, segs), 1)
        result = jnp.zeros((tpl_pad, segs), jnp.float32)
        for s in range(segs):
            b, i = s // block_segs, s % block_segs
            top = jnp.max(acc[b, i * tpl_pad : (i + 1) * tpl_pad, :], axis=1, keepdims=True)
            result = jnp.where(column == s, top, result)
        out_ref[...] = (result / norm).T

    any_vmem = pl.BlockSpec(memory_space=pltpu.VMEM)
    peaks = pl.pallas_call(
        kernel,
        out_shape=jax.ShapeDtypeStruct((segs, tpl_pad), jnp.float32),
        in_specs=[pl.BlockSpec(memory_space=pltpu.HBM)]
        + [any_vmem] * 2
        + [pl.BlockSpec(memory_space=pltpu.HBM)],
        out_specs=any_vmem,
        scratch_shapes=[
            pltpu.SMEM((segs,), jnp.int32),
            pltpu.SemaphoreType.DMA,
            pltpu.SemaphoreType.DMA((2,)),
            pltpu.VMEM((2, tpl_pad, bins + LANES), jnp.float32),
            pltpu.VMEM((segs, 2, bins), jnp.float32),
            pltpu.VMEM((2, segs, bins), jnp.float32),
            pltpu.VMEM((RADIX, rows + 8, span + LANES), jnp.float32),
            pltpu.VMEM((RADIX, rows + 8, span + LANES), jnp.float32),
            pltpu.VMEM((blocks, rows, LANES), jnp.float32),
        ],
        compiler_params=pltpu.CompilerParams(vmem_limit_bytes=VMEM_MIB * 1024 * 1024),
        name="transform",
    )(valid_start, bank, strain, table)
    return peaks[:, :tpl_count]


def by_class(array):
    bins, two, columns = array.shape
    split = array.reshape(bins // RADIX, RADIX, two, columns)
    return split.transpose(3, 1, 2, 0).reshape(columns, two * bins)


def swap(block, axis, bit, dim):
    index = lax.axis_index(axis)
    count = lax.axis_size(axis)
    other = lax.ppermute(block, axis, [(j, j ^ (1 << bit)) for j in range(count)])
    low = jnp.concatenate([block, other], dim)
    high = jnp.concatenate([other, block], dim)
    return jnp.where((index >> bit) & 1 == 0, low, high)


def on_device(spectra, templates, valid_start):
    freq_count = lax.axis_size("freq")
    tpl_count = templates.shape[2] // freq_count
    exchange = lambda a: lax.all_to_all(a, "freq", 0, 0, tiled=True)
    to_all = lambda a: jnp.broadcast_to(a[None], (freq_count,) + a.shape)
    bits = freq_count.bit_length() - 1
    order = [bits - 1] + list(range(bits - 1))
    strain = swap(by_class(spectra)[None], "freq", order[0], 0)
    bank = lax.optimization_barrier(by_class(templates))
    bank = exchange(bank.reshape(freq_count, tpl_count, -1))
    table = make_table(templates.shape[0] * freq_count)
    strain = swap(strain, "freq", order[1], 0)
    for bit in order[2:]:
        strain = swap(strain, "freq", bit, 0)
    for bit in range(lax.axis_size("group").bit_length() - 1):
        strain = swap(strain, "group", bit, 1)
    place = [sum(((f >> bit) & 1) << i for i, bit in enumerate(order)) for f in range(freq_count)]
    peaks = exchange(to_all(transform(bank, strain, place, table, valid_start)))
    return peaks.transpose(0, 2, 1).reshape(templates.shape[2], -1)


def solution(mesh):
    in_specs = (P("freq", None, "group"), P("freq", None, "group"), P())
    out_specs = P("group", None)
    return jax.shard_map(
        on_device, mesh=mesh, in_specs=in_specs, out_specs=out_specs, check_vma=False
    )
```

```python
import functools
import math

import jax
import jax.numpy as jnp
import numpy as np
from jax import lax
from jax.experimental import pallas as pl
from jax.experimental.pallas import tpu as pltpu
from jax.sharding import PartitionSpec as P


N = 4096
RADIX = 8
LANES = 128
VMEM_MIB = 52


def twiddles(bins):
    span = N // RADIX
    rows = bins // RADIX // 16
    t1 = np.arange(span)[None, :]
    fine = (np.arange(16)[:, None] * t1) % span / span
    coarse = (16 * np.arange(rows)[:, None] * t1) % span / span
    low = (np.arange(RADIX)[:, None] * t1) % N / N
    angle = 2.0 * math.pi * np.concatenate([fine, low, coarse], 0)
    return np.stack([np.cos(angle), np.sin(angle)], 1).astype(np.float32)


def make_table(bins):
    per_class = bins // RADIX
    span = N // RADIX
    half = span // 2
    tiles = half // LANES

    def kernel(factor_ref, table, fine):
        for row in range(16):
            for c in range(2):
                fine[c, row : row + 1, :] = factor_ref[row, c : c + 1, :]

        def table_rows(a, carry):
            cr = factor_ref[16 + RADIX + a, 0:1, :]
            ci = factor_ref[16 + RADIX + a, 1:2, :]
            ar = cr * fine[0] - ci * fine[1]
            ai = cr * fine[1] + ci * fine[0]
            at = pl.multiple_of(a * 16, 16)
            for k2 in range(RADIX):
                lr = factor_ref[16 + k2, 0:1, :]
                li = factor_ref[16 + k2, 1:2, :]
                c = (ar * lr - ai * li).astype(jnp.bfloat16)
                s = (ar * li + ai * lr).astype(jnp.bfloat16)
                for ph in range(2):
                    for u in range(tiles):
                        t = slice(ph * half + u * LANES, ph * half + (u + 1) * LANES)
                        table[ph, k2, u, pl.ds(at, 16), :] = c[:, t]
                        table[ph, k2, tiles + u, pl.ds(at, 16), :] = s[:, t]
                        table[ph, k2, u, pl.ds(per_class + at, 16), :] = -s[:, t]
                        table[ph, k2, tiles + u, pl.ds(per_class + at, 16), :] = c[:, t]
            return carry

        lax.fori_loop(0, per_class // 16, table_rows, 0)

    any_vmem = pl.BlockSpec(memory_space=pltpu.VMEM)
    return pl.pallas_call(
        kernel,
        out_shape=jax.ShapeDtypeStruct((2, RADIX, 2 * tiles, 2 * per_class, LANES), jnp.bfloat16),
        in_specs=[any_vmem],
        out_specs=any_vmem,
        scratch_shapes=[pltpu.VMEM((2, 16, span), jnp.float32)],
        compiler_params=pltpu.CompilerParams(vmem_limit_bytes=24 * 1024 * 1024),
        name="table",
    )(jnp.asarray(twiddles(bins)))


def transform(bank, strain, place, table, valid_start):
    sources, tpl_count, local = bank.shape
    segs = strain.shape[1]
    piece = local // (2 * RADIX)
    per_class = sources * piece
    bins = per_class * RADIX
    span = N // RADIX
    half = span // 2
    tpl_pad = -(-tpl_count // 16) * 16
    block_segs = max(d for d in range(1, segs + 1) if segs % (2 * d) == 0 and (d == 1 or d * tpl_pad <= 400))
    blocks = segs // block_segs
    rows = block_segs * tpl_pad
    tiles = per_class // LANES
    if tpl_pad > tpl_count:
        bank = jnp.pad(bank, ((0, 0), (0, tpl_pad - tpl_count), (0, 0)))
    root = np.float32(math.sqrt(0.5))

    def kernel(*refs):
        pl.run_scoped(
            functools.partial(body, *refs),
            pltpu.VMEM((2, RADIX, 2 * half // LANES, 2 * per_class, LANES), jnp.bfloat16),
            pltpu.VMEM((rows, 2 * bins), jnp.bfloat16),
            pltpu.VMEM((rows, 2 * bins), jnp.bfloat16),
        )

    def body(
        start_hbm, bank_ref, strain_ref, table_ref, out_ref, start_ref, start_sem, sem, wide, lines, flat, ya, yb, acc,
        table, xa, xb,
    ):
        loads = [pltpu.make_async_copy(table_ref.at[ph], table.at[ph], sem.at[ph]) for ph in range(2)]
        loads[0].start()
        fetch = pltpu.make_async_copy(start_hbm, start_ref, start_sem)
        fetch.start()

        def gather(source_ref, at_of, count, store):
            lane = lax.broadcasted_iota(jnp.int32, (count, LANES), 1)
            per_tile = LANES // piece
            for j in range(tiles):
                for q in range(local // LANES):
                    parts = [
                        source_ref[at_of[j * per_tile + i], :, q * LANES : (q + 1) * LANES].astype(jnp.float32)
                        for i in range(per_tile)
                    ]
                    for inner in range(0, LANES, piece):
                        value = None
                        for i in range(per_tile):
                            shift = (i * piece - inner) % LANES
                            part = pltpu.roll(parts[i], shift, 1) if shift else parts[i]
                            value = part if value is None else jnp.where(lane >= i * piece, part, value)
                        k2, c = divmod((q * LANES + inner) // piece, 2)
                        store(c, slice(k2 * per_class + j * LANES, k2 * per_class + (j + 1) * LANES), value)

        def store_bank(c, at, value):
            wide[c, :, at] = value

        def store_lines(c, at, value):
            flat[c, :, at] = value

        gather(bank_ref, range(sources), tpl_pad, store_bank)
        gather(strain_ref, place, segs, store_lines)
        for s in range(segs):
            for c in range(2):
                lines[s, c : c + 1, :] = flat[c, s : s + 1, :]

        def cross_piece(x_ref, block, tile):
            k2, j = tile // tiles, tile % tiles
            at = slice(tile * LANES, (tile + 1) * LANES)
            col = k2 * 2 * per_class + j * LANES
            col_im = col + per_class
            d = [
                [jnp.broadcast_to(lines[block * block_segs + i, c : c + 1, at], (8, LANES)) for c in range(2)]
                for i in range(block_segs)
            ]
            shape = (2, 8, LANES)
            for t in range(0, tpl_pad, 16):
                h0 = wide[0, t : t + 16, at].reshape(shape)
                h1 = wide[1, t : t + 16, at].reshape(shape)
                for i in range(block_segs):
                    row = slice(i * tpl_pad + t, i * tpl_pad + t + 16)
                    re = (h0 * d[i][0] + h1 * d[i][1]).reshape(16, LANES)
                    im = (h0 * d[i][1] - h1 * d[i][0]).reshape(16, LANES)
                    x_ref[row, col : col + LANES] = re.astype(jnp.bfloat16)
                    x_ref[row, col_im : col_im + LANES] = im.astype(jnp.bfloat16)

        cross_count = RADIX * tiles
        lane8 = lax.broadcasted_iota(jnp.int32, (8, LANES), 1)
        lane_tiles = half // LANES
        row_tiles = tpl_pad // 8
        peak_count = block_segs * lane_tiles * row_tiles
        signs = {}

        def peak_piece(y_ref, block, phase, index, key):
            i = index // (lane_tiles * row_tiles)
            u = index // row_tiles % lane_tiles
            r = index % row_tiles
            if (key, i, u) not in signs:
                first = start_ref[block * block_segs + i] - (phase * half + u * LANES)
                one = [jnp.float32(1.0), root, jnp.float32(1.0), root]
                signs[key, i, u] = [
                    jnp.where(lane8 >= first - span * j, one[j], -one[j]) for j in range(4)
                ]
            sign = signs[key, i, u]
            row = slice(i * tpl_pad + r * 8, i * tpl_pad + r * 8 + 8)
            re = lambda k: y_ref[k, row, u * LANES : (u + 1) * LANES]
            im = lambda k: y_ref[k, row, half + u * LANES : half + (u + 1) * LANES]

            def four(a, b, c, d):
                ar, ai, br, bi, cr, ci, dr, di = re(a), im(a), re(b), im(b), re(c), im(c), re(d), im(d)
                pr, pi, qr, qi = ar + cr, ai + ci, ar - cr, ai - ci
                sr, si, wr, wi = br + dr, bi + di, br - dr, bi - di
                return (
                    (pr + sr, pi + si),
                    (qr - wi, qi + wr),
                    (pr - sr, pi - si),
                    (qr + wi, qi - wr),
                )

            even = four(0, 2, 4, 6)
            odd = four(1, 3, 5, 7)
            best = None
            for j in range(4):
                er, ei = even[j]
                (a, b), g = odd[j], sign[j]
                if j == 0:
                    yr, yi = er + g * a, ei + g * b
                elif j == 1:
                    yr, yi = er + g * (a - b), ei + g * (a + b)
                elif j == 2:
                    yr, yi = er - g * b, ei + g * a
                else:
                    yr, yi = er - g * (a + b), ei + g * (a - b)
                power = yr * yr + yi * yi
                best = power if best is None else jnp.maximum(best, power)
            if phase == 0 and u == 0:
                acc[block, row, :] = best
            else:
                acc[block, row, :] = jnp.maximum(acc[block, row, :], best)

        for index in range(cross_count):
            cross_piece(xa, 0, index)

        share_p = -(-peak_count // RADIX)
        share_c = -(-(cross_count // 2) // RADIX)
        x_refs, y_refs = (xa, xb), (ya, yb)
        fetch.wait()
        for step in range(2 * blocks):
            block, phase = divmod(step, 2)
            if block == 0:
                loads[phase].wait()
                if phase == 0:
                    loads[1].start()
            signs.clear()
            for k2 in range(RADIX):
                tile = [table[phase, k2, n] for n in range(2 * lane_tiles)]
                y_refs[phase][k2, :rows, :span] = lax.dot_general(
                    x_refs[block % 2][:, k2 * 2 * per_class : (k2 + 1) * 2 * per_class],
                    jnp.concatenate(tile, 1),
                    (((1,), (0,)), ((), ())),
                    preferred_element_type=jnp.float32,
                )
                if step > 0:
                    before, before_phase = divmod(step - 1, 2)
                    for index in range(k2 * share_p, min((k2 + 1) * share_p, peak_count)):
                        peak_piece(y_refs[before_phase], before, before_phase, index, step)
                if block + 1 < blocks:
                    for index in range(k2 * share_c, min((k2 + 1) * share_c, cross_count // 2)):
                        cross_piece(x_refs[(block + 1) % 2], block + 1, phase * (cross_count // 2) + index)
        signs.clear()
        for index in range(peak_count):
            peak_piece(yb, blocks - 1, 1, index, 0)

        square = wide[0, :, :bins] * wide[0, :, :bins] + wide[1, :, :bins] * wide[1, :, :bins]
        norm = jnp.sum(square, axis=1, keepdims=True)
        column = lax.broadcasted_iota(jnp.int32, (tpl_pad, segs), 1)
        result = jnp.zeros((tpl_pad, segs), jnp.float32)
        for s in range(segs):
            b, i = s // block_segs, s % block_segs
            top = jnp.max(acc[b, i * tpl_pad : (i + 1) * tpl_pad, :], axis=1, keepdims=True)
            result = jnp.where(column == s, top, result)
        out_ref[...] = (result / norm).T

    any_vmem = pl.BlockSpec(memory_space=pltpu.VMEM)
    peaks = pl.pallas_call(
        kernel,
        out_shape=jax.ShapeDtypeStruct((segs, tpl_pad), jnp.float32),
        in_specs=[pl.BlockSpec(memory_space=pltpu.HBM)]
        + [any_vmem] * 2
        + [pl.BlockSpec(memory_space=pltpu.HBM)],
        out_specs=any_vmem,
        scratch_shapes=[
            pltpu.SMEM((segs,), jnp.int32),
            pltpu.SemaphoreType.DMA,
            pltpu.SemaphoreType.DMA((2,)),
            pltpu.VMEM((2, tpl_pad, bins + LANES), jnp.float32),
            pltpu.VMEM((segs, 2, bins), jnp.float32),
            pltpu.VMEM((2, segs, bins), jnp.float32),
            pltpu.VMEM((RADIX, rows + 8, span + LANES), jnp.float32),
            pltpu.VMEM((RADIX, rows + 8, span + LANES), jnp.float32),
            pltpu.VMEM((blocks, rows, LANES), jnp.float32),
        ],
        compiler_params=pltpu.CompilerParams(vmem_limit_bytes=VMEM_MIB * 1024 * 1024),
        name="transform",
    )(valid_start, bank, strain, table)
    return peaks[:, :tpl_count]


def by_class(array):
    bins, two, columns = array.shape
    split = array.reshape(bins // RADIX, RADIX, two, columns)
    return split.transpose(3, 1, 2, 0).reshape(columns, two * bins)


def swap(block, axis, bit, dim):
    index = lax.axis_index(axis)
    count = lax.axis_size(axis)
    other = lax.ppermute(block, axis, [(j, j ^ (1 << bit)) for j in range(count)])
    low = jnp.concatenate([block, other], dim)
    high = jnp.concatenate([other, block], dim)
    return jnp.where((index >> bit) & 1 == 0, low, high)


def on_device(spectra, templates, valid_start):
    freq_count = lax.axis_size("freq")
    tpl_count = templates.shape[2] // freq_count
    exchange = lambda a: lax.all_to_all(a, "freq", 0, 0, tiled=True)
    to_all = lambda a: jnp.broadcast_to(a[None], (freq_count,) + a.shape)
    bits = freq_count.bit_length() - 1
    order = [bits - 1] + list(range(bits - 1))
    strain = swap(by_class(spectra)[None], "freq", order[0], 0)
    bank = lax.optimization_barrier(by_class(templates))
    bank = exchange(bank.reshape(freq_count, tpl_count, -1))
    table = make_table(templates.shape[0] * freq_count)
    strain = swap(strain, "freq", order[1], 0)
    for bit in order[2:]:
        strain = swap(strain, "freq", bit, 0)
    for bit in range(lax.axis_size("group").bit_length() - 1):
        strain = swap(strain, "group", bit, 1)
    place = [sum(((f >> bit) & 1) << i for i, bit in enumerate(order)) for f in range(freq_count)]
    peaks = exchange(to_all(transform(bank, strain, place, table, valid_start)))
    return peaks.transpose(0, 2, 1).reshape(templates.shape[2], -1)


def solution(mesh):
    in_specs = (P("freq", None, "group"), P("freq", None, "group"), P())
    out_specs = P("group", None)
    return jax.shard_map(
        on_device, mesh=mesh, in_specs=in_specs, out_specs=out_specs, check_vma=False
    )
```
